32 devices in a mesh: groups: 2 (over y), expert: 16 (over z, x, core).
Axes of the slice: x: 2, y: 2, z: 4, core: 2. Of those that a mesh axis runs over, the one named last changes fastest.
Arguments:
- tokens: bfloat16 [256, 4096], P(('groups', 'expert')), parts along dimension 0, may hold values from -6 to 6
- router: float32 [4096, 8], replicated, may hold values from -0.09375 to 0.09375
- w_gate: bfloat16 [4096, 57344], P(None, 'expert'), may hold values from -0.09375 to 0.09375
- w_up: bfloat16 [4096, 57344], P(None, 'expert'), may hold values from -0.09375 to 0.09375
- w_down: bfloat16 [57344, 4096], P('expert'), may hold values from -0.0625 to 0.0625
- norm_gain: float32 [4096], replicated, may hold values from 0.1 to 1.9
- head_weight: bfloat16 [4096, 16384], P(None, 'expert'), may hold values from -18 to 18
- expert_ids: int32 [256, 2], P(('groups', 'expert')), parts along dimension 0, may hold values from 0 to 7, all different within a row; in each aligned block of 8 rows (0 to 7, 8 to 15, ...) at most 3 rows name the same one
- targets: int32 [256], P(('groups', 'expert')), parts along dimension 0, may hold values from 0 to 16383
- domains: int32 [256], P(('groups', 'expert')), parts along dimension 0, may hold values from 0 to 31
- bins: int32 [256], P(('groups', 'expert')), parts along dimension 0, may hold values from 0 to 15
Outputs:
- hidden_out: bfloat16 [256, 4096], P(('groups', 'expert')), parts along dimension 0
- token_nll: float32 [256], P(('groups', 'expert')), parts along dimension 0
- domain_table: float32 [3, 64, 16], P(None, ('groups', 'expert')), parts along dimension 1
The draws below stay inside these ranges and needn't reach their ends.
There are 2 independent parts, one for each index of `groups`. The reference program is written for one: setup_inputs(seed, part) draws one part's arguments, and reference() takes and returns one part's arrays. A program takes and returns all parts, laid end to end along the dimension named above; an argument that names none is the same for every part. Nothing has to cross between parts.
Inputs may be any that keep to these rules, and one draw needn't show every extreme that they name: `expert_ids`: each token names two different experts. Among the 8 rows of one index of expert, no expert is named more than 3 times, and in some of these blocks one expert is named exactly 3 times.
All inputs are finite; a program needn't handle non-finite values.
Results may differ from the reference program's by a relative error of at most 0.0095.
Values may be sent and summed in bfloat16 or wider, within the bound.
A program may use at most 192 MiB of HBM per device.

```python
import math
import jax
import jax.numpy as jnp
import numpy as np
from jax import lax

D = 4096
FFW = 7168
EXPERTS = 8
VOCAB = 16384
TOK_DEV = 8
BINS = 16
TOKENS = 128
DOMAINS = 32
CAP = 3
N_EXPERT = 16


def draw_head_weight(key, part):
    first_key = jax.random.fold_in(jax.random.fold_in(key, 17), 0)
    values = jax.random.truncated_normal(first_key, -6.0, 6.0, (D, VOCAB), jnp.float32) * D ** (-0.5)
    return values.astype(jnp.bfloat16)


def place_ends(entries, stream_key, least, high):
    extent = entries.shape
    index_at = [jax.random.randint(jax.random.fold_in(stream_key, axis), (), 0, extent[axis]) for axis in range(len(extent))]
    entries = entries.at[tuple(index_at)].set(least)
    longest = extent.index(max(extent))
    index_at[longest] = (index_at[longest] + 1) % extent[longest]
    return entries.at[tuple(index_at)].set(high)


def block_levels(stream_key, dims, shards, least, high):
    def one(axis_at, blocks):
        draws = jax.random.uniform(jax.random.fold_in(jax.random.fold_in(stream_key, 6), axis_at), (blocks,), jnp.float32, least / len(shards), high / len(shards))
        return jnp.repeat(jnp.exp(draws), dims[axis_at] // blocks).reshape((-1,) + (1,) * (len(dims) - axis_at - 1))

    factor_of = one(*shards[0])
    for cut in shards[1:]:
        factor_of = factor_of * one(*cut)
    return factor_of


def rank_table(number_of, slope):
    weights = [(1 << 20) // math.isqrt(grade ** slope) + 1 for grade in range(1, number_of + 1)]
    deviation = 1 + sum(weights) // (1 << 30)
    return np.cumsum(np.array([max(1, weight // deviation) for weight in weights]))


def ranked_ids(own_key, dims, amount, lean):
    grid = rank_table(amount, lean)
    pick = jax.random.randint(jax.random.fold_in(own_key, 1), dims, 0, int(grid[amount - 1]))
    rank = jnp.searchsorted(jnp.asarray(grid, jnp.int32), pick, side="right")
    return jax.random.permutation(jax.random.fold_in(own_key, 2), amount)[rank].astype(jnp.int32)


def routed_block(own_key, own, number, rows, amount, top, bound, slope):
    ranking = jax.random.permutation(own_key, amount)
    crowded, common = shares(amount, rows * top, bound, slope, True), shares(amount, rows * top, bound, slope, False)
    places = jnp.arange(amount)

    def named(sizes, offset_by):
        used = int((sizes > 0).sum())
        fixed = max(1, used // 4)
        moved = fixed + (places - fixed + offset_by * (used - fixed)) % max(1, amount - fixed)
        return jnp.zeros((amount,), jnp.int32).at[ranking[jnp.where(places < fixed, places, moved)]].set(jnp.asarray(sizes, jnp.int32))

    sizes = jnp.where(number % 4 == 0, named(crowded, number // 4), named(common, number - number // 4 - 1))
    mixed = jax.random.permutation(jax.random.fold_in(own, 3), amount)
    source_of, sink = mixed[0:amount // 2 * 2:2], mixed[1:amount // 2 * 2:2]
    slack = jnp.minimum(sizes[source_of] - 1, bound - sizes[sink]) // 2
    slack = jnp.where((source_of == ranking[0]) | (sink == ranking[0]) | (sizes[sink] == 0), 0, jnp.maximum(slack, 0))
    moved = jax.random.randint(jax.random.fold_in(own, 4), (amount // 2,), 0, 1 << 20) % (slack + 1)
    sizes = sizes.at[source_of].add(-moved).at[sink].add(moved)
    members = jnp.searchsorted(jnp.cumsum(sizes), jnp.arange(rows * top), side="right").astype(jnp.int32)
    table = members.reshape(top, rows).T
    table = table[jax.random.permutation(jax.random.fold_in(own, 1), rows)]
    offset_by = jax.random.randint(jax.random.fold_in(own, 2), (rows, 1), 0, top)
    return jnp.take_along_axis(table, (jnp.arange(top)[None, :] + offset_by) % top, axis=1)


def shares(amount, total, bound, skew, full):
    loads = [(1 << 20) // math.isqrt(grade ** skew) + 1 for grade in range(1, amount + 1)]
    largest = bound if full else min(bound, max(-(-total // amount), total * loads[0] // sum(loads)))
    least = 1 if total - largest >= amount - 1 else 0
    given, spare = [largest] + [least] * (amount - 1), total - largest - least * (amount - 1)
    while spare > 0:
        free = [i for i in range(1, amount) if given[i] < largest] or [i for i in range(1, amount) if given[i] < bound]
        whole, left = sum([loads[i] for i in free]), spare
        for i in free:
            addition = min(bound - given[i], max(1, left * loads[i] // whole), spare)
            given[i] = given[i] + addition
            spare = spare - addition
    return np.array(given)


def gaussian(own_key, extent, spread, reach, cuts=(), held_as=jnp.bfloat16):
    entries = spread * jax.random.normal(own_key, extent, jnp.float32)
    if cuts:
        entries = entries * block_levels(own_key, extent, cuts, -0.22, 0.18)
    return jnp.clip(entries, -reach, reach).astype(held_as)


def setup_inputs(seed: int = 0, part: int = 0) -> dict:
    key_list = jax.random.split(jax.random.key(seed), 12)
    part_splits = jax.random.split(jax.random.fold_in(key_list[11], part), 12)
    tokens = gaussian(part_splits[0], (TOKENS, D), 1.0, 6.0, ((0, 16),))
    router = gaussian(key_list[1], (D, EXPERTS), D ** -0.5, 0.09375, (), jnp.float32)
    w_gate = gaussian(key_list[2], (D, EXPERTS * FFW), D ** -0.5, 0.09375, ((1, 16),))
    w_up = gaussian(key_list[3], (D, EXPERTS * FFW), D ** -0.5, 0.09375, ((1, 16),))
    w_down = gaussian(key_list[4], (EXPERTS * FFW, D), FFW ** -0.5, 0.0625, ((0, 16),))
    norm_gain = jnp.clip(1.0 + 0.18 * jax.random.normal(key_list[5], (D,), jnp.float32), 0.1, 1.9)
    head_weight = draw_head_weight(jax.random.fold_in(key_list[11], 71), part)
    expert_ids_keys = jax.random.split(jax.random.fold_in(part_splits[7], 1), TOKENS // TOK_DEV)
    expert_ids_turns = jax.random.permutation(jax.random.fold_in(part_splits[7], 3), TOKENS // TOK_DEV)
    expert_ids = jax.vmap(lambda own, number: routed_block(jax.random.fold_in(part_splits[7], 2), own, number, TOK_DEV, EXPERTS, 2, CAP, 1))(expert_ids_keys, expert_ids_turns).reshape((TOKENS, 2))
    targets = place_ends(jax.random.randint(part_splits[8], (TOKENS,), 0, VOCAB), jax.random.fold_in(part_splits[8], 1), 0, VOCAB - 1).astype(jnp.int32)
    domains = place_ends(ranked_ids(part_splits[9], (TOKENS,), DOMAINS, 2), jax.random.fold_in(part_splits[9], 3), 0, DOMAINS - 1).astype(jnp.int32)
    bins = place_ends(jax.random.randint(part_splits[10], (TOKENS,), 0, BINS), jax.random.fold_in(part_splits[10], 1), 0, BINS - 1).astype(jnp.int32)
    return dict(tokens=tokens, router=router, w_gate=w_gate, w_up=w_up, w_down=w_down, norm_gain=norm_gain, head_weight=head_weight, expert_ids=expert_ids, targets=targets, domains=domains, bins=bins)


def reference(tokens, router, w_gate, w_up, w_down, norm_gain, head_weight, expert_ids, targets, domains, bins):
    highest = lax.Precision.HIGHEST
    per_expert = N_EXPERT // EXPERTS
    group_size = FFW // per_expert
    slot_total = N_EXPERT * CAP
    model_width = tokens.shape[1]
    route_logits = jnp.dot(tokens.astype(jnp.float32), router, precision=highest)
    expert_range = jnp.arange(EXPERTS, dtype=jnp.int32)
    onehot = (expert_ids[:, :, None] == expert_range[None, None, :]).astype(jnp.float32)
    chosen = lax.optimization_barrier(jnp.sum(onehot * route_logits[:, None, :], axis=2))
    gate_weights = jax.nn.sigmoid(chosen - chosen[:, ::-1])
    flat_pairs = onehot.reshape(N_EXPERT, TOK_DEV * 2, EXPERTS)
    before = jnp.cumsum(flat_pairs, axis=1) - flat_pairs
    slot_index = lax.optimization_barrier(jnp.sum(before * flat_pairs, axis=2)).reshape(TOKENS, 2).astype(jnp.int32)
    source_dev = jnp.arange(TOKENS, dtype=jnp.int32) // TOK_DEV
    position = (source_dev[:, None] * CAP + slot_index).astype(jnp.int32)
    pair_rows = jnp.broadcast_to(tokens[:, None, :], (TOKENS, 2, model_width)).reshape(TOKENS * 2, model_width)

    def expert_output(expert_no):
        dest_rows = jnp.where(expert_ids == expert_no, position, slot_total).reshape(-1)
        buffer = jnp.zeros((slot_total, model_width), jnp.bfloat16).at[dest_rows].set(pair_rows, mode='drop')
        gate_cols = lax.dynamic_slice_in_dim(w_gate, expert_no * FFW, FFW, 1)
        up_cols = lax.dynamic_slice_in_dim(w_up, expert_no * FFW, FFW, 1)
        gate_act = jnp.dot(buffer, gate_cols, preferred_element_type=jnp.float32)
        up_act = jnp.dot(buffer, up_cols, preferred_element_type=jnp.float32)
        act = (jax.nn.silu(gate_act) * up_act).astype(jnp.bfloat16)
        down_rows = lax.dynamic_slice_in_dim(w_down, expert_no * FFW, FFW, 0)
        partial_out = jnp.einsum('rgf,gfd->grd', act.reshape(slot_total, per_expert, group_size).astype(jnp.float32), down_rows.reshape(per_expert, group_size, model_width).astype(jnp.float32), precision=highest)
        partial_out = partial_out.astype(jnp.bfloat16)
        return lax.optimization_barrier(jnp.sum(partial_out.astype(jnp.float32), axis=0))
    results = lax.map(expert_output, expert_range)
    picked = results[expert_ids, position]
    moe_out = lax.optimization_barrier(jnp.sum(gate_weights[:, :, None] * picked, axis=1))
    hidden_out = (tokens.astype(jnp.float32) + moe_out).astype(jnp.bfloat16)
    hidden_wide = hidden_out.astype(jnp.float32)
    normed = (hidden_wide * lax.rsqrt(lax.optimization_barrier(jnp.mean(hidden_wide * hidden_wide, axis=1, keepdims=True)) + 1.0) * norm_gain).astype(jnp.bfloat16)
    scores = jnp.dot(normed, head_weight, preferred_element_type=jnp.float32)
    row_top = lax.optimization_barrier(jnp.max(scores, axis=1, keepdims=True))
    exp_scores = jnp.exp(scores - row_top)
    mass_sum = lax.optimization_barrier(jnp.sum(exp_scores, axis=1))
    log_norm = row_top[:, 0] + jnp.log(mass_sum)
    entropy = log_norm - lax.optimization_barrier(jnp.sum(exp_scores * scores, axis=1)) / mass_sum
    target_score = jnp.take_along_axis(scores, targets[:, None].astype(jnp.int32), axis=1)[:, 0]
    token_nll = log_norm - target_score
    dom_hot = (domains[:, None] == jnp.arange(DOMAINS, dtype=jnp.int32)[None, :]).astype(jnp.float32)
    bin_hot = (bins[:, None] == jnp.arange(BINS, dtype=jnp.int32)[None, :]).astype(jnp.float32)
    columns = jnp.stack([jnp.ones_like(token_nll), token_nll, entropy], axis=1)
    spread_cols = (columns[:, :, None] * bin_hot[:, None, :]).reshape(TOKENS, 3 * BINS)
    table = jnp.dot(dom_hot.T, spread_cols, precision=highest)
    domain_table = table.reshape(DOMAINS, 3, BINS).transpose(1, 0, 2)
    return (hidden_out, token_nll, domain_table)
```

```python
import functools
import jax
import jax.numpy as jnp
from jax import lax
from jax.experimental import pallas as pl
from jax.experimental.pallas import tpu as pltpu
from jax.sharding import PartitionSpec as P

EXPERTS = 8
DOM_DEV = 2
BINS = 16
CAP = 3
PAD = 4
F32 = jnp.float32
BF16 = jnp.bfloat16
HIGHEST = lax.Precision.HIGHEST


def iota(shape, dim):
    return lax.broadcasted_iota(jnp.int32, shape, dim)


def kernel(cfg, tokens, ids_row, meta, router_t, gain, w_gate, w_up, w_down, head,
           out_hidden, out_stats,
           gu_buf, dn_buf, hd_buf, send_d, recv_d, x_buf, act_buf, p_buf, r1_buf, s_buf, r2_buf,
           h_buf, meta_buf, st_send, st_buf, scores, ssq, wt_buf,
           gu_sem, dn_sem, hd_sem, own_sem, d1_send, d1_recv, d2_send, d2_recv, r1_send, r1_recv,
           r2_send, r2_recv, ag_send, ag_recv, mt_send, mt_recv, st_ssem, st_rsem):
    n, G, C, X, Z = cfg["n"], cfg["G"], cfg["C"], cfg["X"], cfg["Z"]
    rows, D = tokens.shape
    half = D // 2
    E = EXPERTS
    TF, NF, NGU = cfg["TF"], cfg["NF"], cfg["NGU"]
    TD, ND, NDW = cfg["TD"], cfg["ND"], cfg["NDW"]
    NCH = cfg["NCH"]
    Nc = D // NCH
    hc = Nc // 2
    per_chunk = ND // NCH
    me = lax.axis_index("expert")
    me_e, me_g = me // G, me % G
    mz, mx, mc = me // (C * X), (me // C) % X, me % C
    my_place = (mc * X + mx) * Z + mz

    def remote(src, dst, ss, rs, peer):
        return pltpu.make_async_remote_copy(
            src_ref=src, dst_ref=dst, send_sem=ss, recv_sem=rs,
            device_id={"expert": peer}, device_id_type=pl.DeviceIdType.MESH)

    def drain(ref, sem):
        pltpu.make_async_copy(ref, ref, sem).wait()

    def gu_copy(t, src, which, slot):
        return pltpu.make_async_copy(
            src.at[:, pl.ds(pl.multiple_of(t * TF, TF if TF % 128 == 0 else 1), TF)] if NF > 1 else src,
            gu_buf.at[slot, which], gu_sem.at[slot, which])

    def gu_start(t, slot):
        gu_copy(t, w_gate, 0, slot).start()
        gu_copy(t, w_up, 1, slot).start()

    def dn_copy(t, slot):
        return pltpu.make_async_copy(
            w_down.at[:, pl.ds(t * TD, TD)], dn_buf.at[slot], dn_sem.at[slot])

    def hd_copy(c):
        return pltpu.make_async_copy(head.at[pl.ds(c * Nc, Nc)], hd_buf.at[c], hd_sem.at[c])

    for t in range(NGU):
        gu_start(t, t)
    barrier = pltpu.get_barrier_semaphore()

    def greet(o, carry):
        pl.semaphore_signal(barrier, inc=1, device_id={"expert": (me + o) % n},
                            device_id_type=pl.DeviceIdType.MESH)
        return carry

    lax.fori_loop(1, n, greet, 0)
    for t in range(NDW):
        dn_copy(t, t).start()

    RB = E * 2 * PAD
    r = iota((RB, rows), 0)
    r_e, r_h, r_s = r // (2 * PAD), (r % (2 * PAD)) // PAD, r % PAD
    member = ((ids_row[0:1, :] == r_e) | (ids_row[1:2, :] == r_e)).astype(F32)
    upper = (iota((rows, rows), 0) < iota((rows, rows), 1)).astype(F32)
    slot = jnp.dot(member, upper, preferred_element_type=F32)
    lay = member * (slot == r_s.astype(F32)).astype(F32)
    lay_lo = (lay * (r_h == 0).astype(F32)).astype(BF16)
    lay_hi = (lay * (r_h == 1).astype(F32)).astype(BF16)
    packed = (jnp.dot(lay_lo, tokens[:, :half], preferred_element_type=F32)
              + jnp.dot(lay_hi, tokens[:, half:], preferred_element_type=F32))
    send_d[...] = packed.reshape(E, 2 * PAD, half).astype(BF16)
    meta_buf[my_place] = meta[...]

    pl.semaphore_wait(barrier, n - 1)

    d1 = []
    for o in range(1, E):
        e = (me_e + o) % E
        cp = remote(send_d.at[e], recv_d.at[me_g, me_e], d1_send.at[o], d1_recv.at[o], e * G + me_g)
        cp.start()
        d1.append(cp)
    own = pltpu.make_async_copy(send_d.at[me_e], recv_d.at[me_g, me_e], own_sem)
    own.start()

    def meta_send(o, carry):
        remote(meta, meta_buf.at[my_place], mt_send, mt_recv, (me + o) % n).start()
        return carry

    tok32 = tokens[...].astype(F32)
    ids0, ids1 = meta[:, 0:1], meta[:, 1:2]
    c0 = jnp.zeros((rows, 1), F32)
    c1 = jnp.zeros((rows, 1), F32)
    for e in range(E):
        logit = jnp.sum(tok32 * router_t[e:e + 1, :], axis=1, keepdims=True)
        c0 = c0 + jnp.where(ids0 == e, logit, 0.0)
        c1 = c1 + jnp.where(ids1 == e, logit, 0.0)
    g0 = 1.0 / (1.0 + jnp.exp(c1 - c0))
    g1 = 1.0 / (1.0 + jnp.exp(c0 - c1))
    q = iota((rows, RB), 1)
    q_e, q_h, q_s = q // (2 * PAD), (q % (2 * PAD)) // PAD, q % PAD
    is0, is1 = ids0 == q_e, ids1 == q_e
    member_t = (is0 | is1).astype(F32)
    lower = (iota((rows, rows), 1) < iota((rows, rows), 0)).astype(F32)
    slot_t = jnp.dot(lower, member_t, preferred_element_type=F32)
    weight = (jnp.where(is0, g0, 0.0) + jnp.where(is1, g1, 0.0)) * (
        slot_t == q_s.astype(F32)).astype(F32)
    wt_buf[0] = weight * (q_h == 0).astype(F32)
    wt_buf[1] = weight * (q_h == 1).astype(F32)

    own.wait()
    d2 = []
    for o in range(E):
        e = (me_e - o + E) % E
        if o > 0:
            d1[o - 1].wait_recv()
        for k in range(1, G):
            cp = remote(recv_d.at[me_g, e], recv_d.at[me_g, e], d2_send.at[k], d2_recv.at[k],
                        me_e * G + (me_g + k) % G)
            cp.start()
    for k in range(1, G):
        drain(recv_d.at[(me_g - k + G) % G], d2_recv.at[k])

    M = n * PAD
    pick_r, pick_c = iota((M, n * 2 * PAD), 0), iota((M, n * 2 * PAD), 1)
    base = (pick_r // PAD) * (2 * PAD) + pick_r % PAD
    sel_lo = (pick_c == base).astype(BF16)
    sel_hi = (pick_c == base + PAD).astype(BF16)
    W = 512
    for j in range(half // W):
        got = recv_d[:, :, :, j * W:(j + 1) * W].astype(F32).reshape(n * 2 * PAD, W).astype(BF16)
        x_buf[:, j * W:(j + 1) * W] = jnp.dot(
            sel_lo, got, preferred_element_type=F32).astype(BF16)
        x_buf[:, half + j * W:half + (j + 1) * W] = jnp.dot(
            sel_hi, got, preferred_element_type=F32).astype(BF16)

    lax.fori_loop(1, n, meta_send, 0)

    def expert_tile(t, carry):
        s = t % NGU
        gu_copy(t, w_gate, 0, s).wait()
        g = jnp.dot(x_buf[...], gu_buf[s, 0], preferred_element_type=F32)
        gu_copy(t, w_up, 1, s).wait()
        u = jnp.dot(x_buf[...], gu_buf[s, 1], preferred_element_type=F32)
        a = (g / (1.0 + jnp.exp(-g)) * u).astype(BF16)
        act_buf[t] = a

        @pl.when(t + NGU < NF)
        def _():
            gu_start(t + NGU, s)

        return carry

    lax.fori_loop(0, NF, expert_tile, 0)
    for c in range(NCH):
        hd_copy(c).start()

    br = iota((RB, E * PAD), 0)
    bc = iota((RB, E * PAD), 1)
    b_src = (br // (2 * PAD)) * PAD + br % PAD
    b_h = (br % (2 * PAD)) // PAD
    blk_lo = ((bc == b_src) & (b_h == 0)).astype(BF16)
    blk_hi = ((bc == b_src) & (b_h == 1)).astype(BF16)

    def down(c):
        for i in range(per_chunk):
            t = c * per_chunk + i
            s = t % NDW
            dn_copy(t, s).wait()
            acc = jnp.dot(act_buf[0], dn_buf[s, 0:TF], preferred_element_type=F32)
            for f in range(1, NF):
                acc = acc + jnp.dot(act_buf[f], dn_buf[s, f * TF:(f + 1) * TF],
                                    preferred_element_type=F32)
            p_buf[c, :, :, i * TD:(i + 1) * TD] = acc.astype(BF16).reshape(G, E * PAD, TD)
            if t + NDW < ND:
                dn_copy(t + NDW, s).start()
        for k in range(1, G):
            remote(p_buf.at[c, (me_g + k) % G], r1_buf.at[c, k], r1_send.at[c, k], r1_recv.at[c, k],
                   me_e * G + (me_g + k) % G).start()

    def stage2(c):
        total = p_buf[c, me_g].astype(F32)
        for k in range(1, G):
            drain(r1_buf.at[c, k], r1_recv.at[c, k])
            total = total + r1_buf[c, k].astype(F32)
        summed = total.astype(BF16)
        block = (jnp.dot(blk_lo, summed[:, :hc], preferred_element_type=F32)
                 + jnp.dot(blk_hi, summed[:, hc:], preferred_element_type=F32))
        s_buf[c] = block.reshape(E, 2 * PAD, hc).astype(BF16)
        r2_buf[c, me_e] = s_buf[c, me_e]
        for o in range(1, E):
            e = (me_e + o) % E
            remote(s_buf.at[c, e], r2_buf.at[c, me_e], r2_send.at[c], r2_recv.at[c],
                   e * G + me_g).start()

    def stage3(c):
        drain(r2_buf.at[c, pl.ds(0, E - 1)], r2_recv.at[c])
        got = r2_buf[c].astype(F32).reshape(RB, hc)
        at = c * Nc
        for h in range(2):
            moe = jnp.dot(wt_buf[h], got, precision=HIGHEST, preferred_element_type=F32)
            lo = at + h * hc
            hid = (tokens[:, lo:lo + hc].astype(F32) + moe).astype(BF16)
            out_hidden[:, lo:lo + hc] = hid
            h_buf[c, mc, mx, mz, :, h * hc:(h + 1) * hc] = hid
        src = h_buf.at[c, mc, mx, mz]
        for o in range(1, Z):
            remote(src, src, ag_send.at[c, 0], ag_recv.at[c, 0],
                   (((mz + o) % Z) * X + mx) * C + mc).start()

    def gather2(c):
        drain(h_buf.at[c, mc, mx, pl.ds(0, Z - 1)], ag_recv.at[c, 0])
        src = h_buf.at[c, mc, mx]
        for o in range(1, X):
            remote(src, src, ag_send.at[c, 1], ag_recv.at[c, 1],
                   (mz * X + (mx + o) % X) * C + mc).start()

    def gather3(c):
        drain(h_buf.at[c, mc, pl.ds(0, X - 1)], ag_recv.at[c, 1])
        src = h_buf.at[c, mc]
        for o in range(1, C):
            remote(src, src, ag_send.at[c, 2], ag_recv.at[c, 2],
                   (mz * X + mx) * C + (mc + o) % C).start()

    def head_part(c):
        drain(h_buf.at[c, pl.ds(0, C - 1)], ag_recv.at[c, 2])
        wide = h_buf[c].astype(F32).reshape(n * rows, Nc)
        sq = jnp.sum(wide * wide, axis=1, keepdims=True)
        scaled = (wide * gain[:, c * Nc:(c + 1) * Nc]).astype(BF16)
        hd_copy(c).wait()
        part = jnp.dot(scaled, hd_buf[c], preferred_element_type=F32)
        if c == 0:
            scores[...] = part
            ssq[...] = sq
        else:
            scores[...] += part
            ssq[...] += sq

    stages = [(down, 0.0), (stage2, 2.1), (stage3, 6.1), (gather2, 9.1), (gather3, 11.1), (head_part, 13.1)]
    plan = []
    for c in range(NCH):
        for at, (fn, when) in enumerate(stages):
            plan.append((2.0 * c + when, at, c, fn))
    for _, _, c, fn in sorted(plan, key=lambda item: item[:3]):
        fn(c)

    drain(meta_buf.at[pl.ds(0, n - 1)], mt_recv)
    R = n * rows
    V = scores.shape[1]
    sc = scores[...] * lax.rsqrt(ssq[...] * (1.0 / D) + 1.0)
    ids = meta_buf[...].reshape(R, 128)
    top = jnp.max(sc, axis=1, keepdims=True)
    ex = jnp.exp(sc - top)
    mass = jnp.sum(ex, axis=1, keepdims=True)
    moment = jnp.sum(ex * sc, axis=1, keepdims=True)
    column = iota((R, V), 1) + me * V
    hit = jnp.sum(jnp.where(ids[:, 2:3] == column, sc, 0.0), axis=1, keepdims=True)
    lane = iota((R, 128), 1)
    stat = jnp.where(lane == 0, top, jnp.where(lane == 1, mass, jnp.where(
        lane == 2, moment, jnp.where(lane == 3, hit, 0.0))))
    turned = stat.T[0:8, :]
    st_send[...] = turned
    st_buf[me] = turned

    def stat_send(o, carry):
        remote(st_send, st_buf.at[me], st_ssem, st_rsem, (me + o) % n).start()
        return carry

    lax.fori_loop(1, n, stat_send, 0)

    dom, bins = ids[:, 3:4], ids[:, 4:5]
    col = iota((R, 128), 1)
    spot = (dom - me * DOM_DEV) * BINS + bins
    inside = (dom >= me * DOM_DEV) & (dom < (me + 1) * DOM_DEV)
    own_row = my_place * rows
    hot = ((inside & (col == spot)) | (
        (col >= 64) & (col < 64 + rows) & (iota((R, 128), 0) == own_row + col - 64))).astype(F32)

    for cp in d1:
        cp.wait_send()
    for k in range(1, G):
        drain(recv_d.at[me_g], d2_send.at[k])
    for c in range(NCH):
        for k in range(1, G):
            drain(r1_buf.at[c, k], r1_send.at[c, k])
        drain(r2_buf.at[c, pl.ds(0, E - 1)], r2_send.at[c])
        drain(h_buf.at[c, mc, mx, pl.ds(0, Z - 1)], ag_send.at[c, 0])
        drain(h_buf.at[c, mc, pl.ds(0, X - 1)], ag_send.at[c, 1])
        drain(h_buf.at[c, pl.ds(0, C - 1)], ag_send.at[c, 2])
    drain(meta_buf.at[pl.ds(0, n - 1)], mt_send)
    drain(st_buf.at[pl.ds(0, n - 1)], st_ssem)
    drain(st_buf.at[pl.ds(0, n - 1)], st_rsem)
    tops = st_buf[:, 0, :]
    joined = jnp.max(tops, axis=0, keepdims=True)
    factor = jnp.exp(tops - joined)
    mass_all = jnp.sum(st_buf[:, 1, :] * factor, axis=0, keepdims=True)
    moment_all = jnp.sum(st_buf[:, 2, :] * factor, axis=0, keepdims=True)
    target = jnp.sum(st_buf[:, 3, :], axis=0, keepdims=True)
    log_norm = joined + jnp.log(mass_all)
    nll = log_norm - target
    ent = log_norm - moment_all / mass_all
    kind = iota((8, R), 0)
    vals = jnp.where(kind == 0, 1.0, jnp.where(kind == 1, nll, jnp.where(kind == 2, ent, 0.0)))
    out_stats[...] = jnp.dot(vals, hot, precision=HIGHEST, preferred_element_type=F32)


def on_device(tokens, router, w_gate, w_up, w_down, norm_gain, head_weight, expert_ids, targets,
              domains, bins):
    n = lax.axis_size("expert")
    rows, D = tokens.shape
    F = w_down.shape[0]
    V = head_weight.shape[1]
    G = n // EXPERTS
    C, X = 2, 2
    Z = n // (C * X)
    TF = 512 if F % 512 == 0 else F
    NF = F // TF
    TD = 512
    ND = D // TD
    NCH = 4
    cfg = dict(n=n, G=G, C=C, X=X, Z=Z, TF=TF, NF=NF, NGU=min(3, NF), TD=TD, ND=ND,
               NDW=min(5, ND), NCH=NCH)
    Nc = D // NCH
    hc = Nc // 2
    lane = jnp.arange(128, dtype=jnp.int32)[None, :]
    meta = jnp.where(lane == 0, expert_ids[:, 0:1], jnp.where(
        lane == 1, expert_ids[:, 1:2], jnp.where(
            lane == 2, targets[:, None], jnp.where(
                lane == 3, domains[:, None], jnp.where(lane == 4, bins[:, None], 0)))))
    vmem = pl.BlockSpec(memory_space=pltpu.VMEM)
    hbm = pl.BlockSpec(memory_space=pltpu.HBM)
    DMA = pltpu.SemaphoreType.DMA
    M = n * PAD
    scratch = [
        pltpu.VMEM((cfg["NGU"], 2, D, TF), BF16),
        pltpu.VMEM((cfg["NDW"], F, TD), BF16),
        pltpu.VMEM((NCH, Nc, V), BF16),
        pltpu.VMEM((EXPERTS, 2 * PAD, D // 2), BF16),
        pltpu.VMEM((G, EXPERTS, 2 * PAD, D // 2), BF16),
        pltpu.VMEM((M, D), BF16),
        pltpu.VMEM((NF, M, TF), BF16),
        pltpu.VMEM((NCH, G, EXPERTS * PAD, Nc), BF16),
        pltpu.VMEM((NCH, G, EXPERTS * PAD, Nc), BF16),
        pltpu.VMEM((NCH, EXPERTS, 2 * PAD, hc), BF16),
        pltpu.VMEM((NCH, EXPERTS, 2 * PAD, hc), BF16),
        pltpu.VMEM((NCH, C, X, Z, rows, Nc), BF16),
        pltpu.VMEM((n, rows, 128), jnp.int32),
        pltpu.VMEM((8, n * rows), F32),
        pltpu.VMEM((n, 8, n * rows), F32),
        pltpu.VMEM((n * rows, V), F32),
        pltpu.VMEM((n * rows, 1), F32),
        pltpu.VMEM((2, rows, EXPERTS * 2 * PAD), F32),
        DMA((cfg["NGU"], 2)), DMA((cfg["NDW"],)), DMA((NCH,)), DMA(()),
        DMA((EXPERTS,)), DMA((EXPERTS,)), DMA((G,)), DMA((G,)),
        DMA((NCH, G)), DMA((NCH, G)), DMA((NCH,)), DMA((NCH,)),
        DMA((NCH, 3)), DMA((NCH, 3)), DMA(()), DMA(()), DMA(()), DMA(()),
    ]
    hidden, stats = pl.pallas_call(
        functools.partial(kernel, cfg),
        out_shape=(jax.ShapeDtypeStruct((rows, D), BF16), jax.ShapeDtypeStruct((8, 128), F32)),
        in_specs=[vmem] * 5 + [hbm] * 4,
        out_specs=(vmem, vmem),
        scratch_shapes=scratch,
        compiler_params=pltpu.CompilerParams(
            collective_id=0, has_side_effects=True, vmem_limit_bytes=67043328),
    )(tokens, expert_ids.T, meta, router.T, norm_gain[None, :], w_gate, w_up, w_down, head_weight)
    token_nll = stats[1, 64:64 + rows]
    domain_table = stats[0:3, 0:DOM_DEV * BINS].reshape(3, DOM_DEV, BINS)
    return hidden, token_nll, domain_table


def solution(mesh):
    return jax.shard_map(
        on_device,
        mesh=mesh,
        in_specs=(
            P(("groups", "expert"), None),
            P(),
            P(None, "expert"),
            P(None, "expert"),
            P("expert", None),
            P(),
            P(None, "expert"),
            P(("groups", "expert"), None),
            P(("groups", "expert")),
            P(("groups", "expert")),
            P(("groups", "expert")),
        ),
        out_specs=(
            P(("groups", "expert"), None),
            P(("groups", "expert")),
            P(None, ("groups", "expert"), None),
        ),
        check_vma=False,
    )
```

```python
import functools
import jax
import jax.numpy as jnp
from jax import lax
from jax.experimental import pallas as pl
from jax.experimental.pallas import tpu as pltpu
from jax.sharding import PartitionSpec as P

EXPERTS = 8
DOM_DEV = 2
BINS = 16
CAP = 3
PAD = 4
F32 = jnp.float32
BF16 = jnp.bfloat16
HIGHEST = lax.Precision.HIGHEST


def iota(shape, dim):
    return lax.broadcasted_iota(jnp.int32, shape, dim)


def kernel(cfg, tokens, ids_row, tgt_row, dom_row, bin_row, router_t, gain, w_gate, w_up, w_down,
           head, out_hidden, out_nll, out_table,
           gu_buf, dn_buf, hd_buf, send_d, recv_d, x_buf, act_buf, p_buf, r1_buf, s_buf, r2_buf,
           h_buf, meta_buf, st_send, st_buf, scores, ssq, wt_buf,
           gu_sem, dn_sem, hd_sem, own_sem, d1_send, d1_recv, d2_send, d2_recv, r1_send, r1_recv,
           r2_send, r2_recv, ag_send, ag_recv, mt_send, mt_recv, st_ssem, st_rsem):
    n, G, C, X, Z = cfg["n"], cfg["G"], cfg["C"], cfg["X"], cfg["Z"]
    rows, D = tokens.shape
    half = D // 2
    E = EXPERTS
    TF, NF, NGU = cfg["TF"], cfg["NF"], cfg["NGU"]
    TD, ND, NDW = cfg["TD"], cfg["ND"], cfg["NDW"]
    NCH = cfg["NCH"]
    Nc = D // NCH
    hc = Nc // 2
    per_chunk = ND // NCH
    me = lax.axis_index("expert")
    me_e, me_g = me // G, me % G
    mz, mx, mc = me // (C * X), (me // C) % X, me % C
    my_place = (mc * X + mx) * Z + mz

    def remote(src, dst, ss, rs, peer):
        return pltpu.make_async_remote_copy(
            src_ref=src, dst_ref=dst, send_sem=ss, recv_sem=rs,
            device_id={"expert": peer}, device_id_type=pl.DeviceIdType.MESH)

    def drain(ref, sem):
        pltpu.make_async_copy(ref, ref, sem).wait()

    def gu_copy(t, src, which, slot):
        return pltpu.make_async_copy(
            src.at[:, pl.ds(pl.multiple_of(t * TF, TF if TF % 128 == 0 else 1), TF)] if NF > 1 else src,
            gu_buf.at[slot, which], gu_sem.at[slot, which])

    def gu_start(t, slot):
        gu_copy(t, w_gate, 0, slot).start()
        gu_copy(t, w_up, 1, slot).start()

    def dn_copy(t, slot):
        return pltpu.make_async_copy(
            w_down.at[:, pl.ds(t * TD, TD)], dn_buf.at[slot], dn_sem.at[slot])

    def hd_copy(c):
        return pltpu.make_async_copy(head.at[pl.ds(c * Nc, Nc)], hd_buf.at[c], hd_sem.at[c])

    for t in range(NGU):
        gu_start(t, t)
    barrier = pltpu.get_barrier_semaphore()

    def greet(o, carry):
        pl.semaphore_signal(barrier, inc=1, device_id={"expert": (me + o) % n},
                            device_id_type=pl.DeviceIdType.MESH)
        return carry

    lax.fori_loop(1, n, greet, 0)
    for t in range(NDW):
        dn_copy(t, t).start()

    RB = E * 2 * PAD
    r = iota((RB, rows), 0)
    r_e, r_h, r_s = r // (2 * PAD), (r % (2 * PAD)) // PAD, r % PAD
    member = ((ids_row[0:1, :] == r_e) | (ids_row[1:2, :] == r_e)).astype(F32)
    upper = (iota((rows, rows), 0) < iota((rows, rows), 1)).astype(F32)
    slot = jnp.dot(member, upper, preferred_element_type=F32)
    lay = member * (slot == r_s.astype(F32)).astype(F32)
    lay_lo = (lay * (r_h == 0).astype(F32)).astype(BF16)
    lay_hi = (lay * (r_h == 1).astype(F32)).astype(BF16)
    packed = (jnp.dot(lay_lo, tokens[:, :half], preferred_element_type=F32)
              + jnp.dot(lay_hi, tokens[:, half:], preferred_element_type=F32))
    send_d[...] = packed.reshape(E, 2 * PAD, half).astype(BF16)
    eye = iota((rows, rows), 0) == iota((rows, rows), 1)

    def column_of(row):
        wide = jnp.where(eye, row.astype(F32), 0.0)
        return jnp.sum(wide, axis=1, keepdims=True).astype(jnp.int32)

    ids0, ids1 = column_of(ids_row[0:1, :]), column_of(ids_row[1:2, :])
    ml = iota((rows, 128), 1)
    meta_buf[my_place] = jnp.where(ml == 2, column_of(tgt_row[...]), jnp.where(
        ml == 3, column_of(dom_row[...]), jnp.where(ml == 4, column_of(bin_row[...]), 0)))

    pl.semaphore_wait(barrier, n - 1)

    d1 = []
    for o in range(1, E):
        e = (me_e + o) % E
        cp = remote(send_d.at[e], recv_d.at[me_g, me_e], d1_send.at[o], d1_recv.at[o], e * G + me_g)
        cp.start()
        d1.append(cp)
    own = pltpu.make_async_copy(send_d.at[me_e], recv_d.at[me_g, me_e], own_sem)
    own.start()

    def meta_send(o, carry):
        remote(meta_buf.at[my_place], meta_buf.at[my_place], mt_send, mt_recv, (me + o) % n).start()
        return carry

    tok32 = tokens[...].astype(F32)
    c0 = jnp.zeros((rows, 1), F32)
    c1 = jnp.zeros((rows, 1), F32)
    for e in range(E):
        logit = jnp.sum(tok32 * router_t[e:e + 1, :], axis=1, keepdims=True)
        c0 = c0 + jnp.where(ids0 == e, logit, 0.0)
        c1 = c1 + jnp.where(ids1 == e, logit, 0.0)
    g0 = 1.0 / (1.0 + jnp.exp(c1 - c0))
    g1 = 1.0 / (1.0 + jnp.exp(c0 - c1))
    q = iota((rows, RB), 1)
    q_e, q_h, q_s = q // (2 * PAD), (q % (2 * PAD)) // PAD, q % PAD
    is0, is1 = ids0 == q_e, ids1 == q_e
    member_t = (is0 | is1).astype(F32)
    lower = (iota((rows, rows), 1) < iota((rows, rows), 0)).astype(F32)
    slot_t = jnp.dot(lower, member_t, preferred_element_type=F32)
    weight = (jnp.where(is0, g0, 0.0) + jnp.where(is1, g1, 0.0)) * (
        slot_t == q_s.astype(F32)).astype(F32)
    wt_buf[0] = weight * (q_h == 0).astype(F32)
    wt_buf[1] = weight * (q_h == 1).astype(F32)

    own.wait()
    d2 = []
    for o in range(E):
        e = (me_e - o + E) % E
        if o > 0:
            d1[o - 1].wait_recv()
        for k in range(1, G):
            cp = remote(recv_d.at[me_g, e], recv_d.at[me_g, e], d2_send.at[k], d2_recv.at[k],
                        me_e * G + (me_g + k) % G)
            cp.start()
    for k in range(1, G):
        drain(recv_d.at[(me_g - k + G) % G], d2_recv.at[k])

    M = n * PAD
    pick_r, pick_c = iota((M, n * 2 * PAD), 0), iota((M, n * 2 * PAD), 1)
    base = (pick_r // PAD) * (2 * PAD) + pick_r % PAD
    sel_lo = (pick_c == base).astype(BF16)
    sel_hi = (pick_c == base + PAD).astype(BF16)
    W = 512
    for j in range(half // W):
        got = recv_d[:, :, :, j * W:(j + 1) * W].astype(F32).reshape(n * 2 * PAD, W).astype(BF16)
        x_buf[:, j * W:(j + 1) * W] = jnp.dot(
            sel_lo, got, preferred_element_type=F32).astype(BF16)
        x_buf[:, half + j * W:half + (j + 1) * W] = jnp.dot(
            sel_hi, got, preferred_element_type=F32).astype(BF16)

    lax.fori_loop(1, n, meta_send, 0)

    def expert_tile(t, carry):
        s = t % NGU
        gu_copy(t, w_gate, 0, s).wait()
        g = jnp.dot(x_buf[...], gu_buf[s, 0], preferred_element_type=F32)
        gu_copy(t, w_up, 1, s).wait()
        u = jnp.dot(x_buf[...], gu_buf[s, 1], preferred_element_type=F32)
        a = (g / (1.0 + jnp.exp(-g)) * u).astype(BF16)
        act_buf[t] = a

        @pl.when(t + NGU < NF)
        def _():
            gu_start(t + NGU, s)

        return carry

    lax.fori_loop(0, NF, expert_tile, 0)

    br = iota((RB, E * PAD), 0)
    bc = iota((RB, E * PAD), 1)
    b_src = (br // (2 * PAD)) * PAD + br % PAD
    b_h = (br % (2 * PAD)) // PAD
    blk_lo = ((bc == b_src) & (b_h == 0)).astype(BF16)
    blk_hi = ((bc == b_src) & (b_h == 1)).astype(BF16)

    def down(c):
        for i in range(per_chunk):
            t = c * per_chunk + i
            s = t % NDW
            dn_copy(t, s).wait()
            acc = jnp.dot(act_buf[0], dn_buf[s, 0:TF], preferred_element_type=F32)
            for f in range(1, NF):
                acc = acc + jnp.dot(act_buf[f], dn_buf[s, f * TF:(f + 1) * TF],
                                    preferred_element_type=F32)
            p_buf[c, :, :, i * TD:(i + 1) * TD] = acc.astype(BF16).reshape(G, E * PAD, TD)
            if t + NDW < ND:
                dn_copy(t + NDW, s).start()
            if t + 1 == max(ND - NDW, 1):
                for h in range(NCH):
                    hd_copy(h).start()
        for k in range(1, G):
            remote(p_buf.at[c, (me_g + k) % G], r1_buf.at[c, k], r1_send.at[c, k], r1_recv.at[c, k],
                   me_e * G + (me_g + k) % G).start()

    def stage2(c):
        total = p_buf[c, me_g].astype(F32)
        for k in range(1, G):
            drain(r1_buf.at[c, k], r1_recv.at[c, k])
            total = total + r1_buf[c, k].astype(F32)
        summed = total.astype(BF16)
        block = (jnp.dot(blk_lo, summed[:, :hc], preferred_element_type=F32)
                 + jnp.dot(blk_hi, summed[:, hc:], preferred_element_type=F32))
        s_buf[c] = block.reshape(E, 2 * PAD, hc).astype(BF16)
        r2_buf[c, me_e] = s_buf[c, me_e]
        for o in range(1, E):
            e = (me_e + o) % E
            remote(s_buf.at[c, e], r2_buf.at[c, me_e], r2_send.at[c], r2_recv.at[c],
                   e * G + me_g).start()

    def stage3(c):
        drain(r2_buf.at[c, pl.ds(0, E - 1)], r2_recv.at[c])
        got = r2_buf[c].astype(F32).reshape(RB, hc)
        at = c * Nc
        for h in range(2):
            moe = jnp.dot(wt_buf[h], got, precision=HIGHEST, preferred_element_type=F32)
            lo = at + h * hc
            hid = (tokens[:, lo:lo + hc].astype(F32) + moe).astype(BF16)
            out_hidden[:, lo:lo + hc] = hid
            h_buf[c, mc, mx, mz, :, h * hc:(h + 1) * hc] = hid
        src = h_buf.at[c, mc, mx, mz]
        for o in range(1, Z):
            remote(src, src, ag_send.at[c, 0], ag_recv.at[c, 0],
                   (((mz + o) % Z) * X + mx) * C + mc).start()

    def gather2(c):
        drain(h_buf.at[c, mc, mx, pl.ds(0, Z - 1)], ag_recv.at[c, 0])
        src = h_buf.at[c, mc, mx]
        for o in range(1, X):
            remote(src, src, ag_send.at[c, 1], ag_recv.at[c, 1],
                   (mz * X + (mx + o) % X) * C + mc).start()

    def gather3(c):
        drain(h_buf.at[c, mc, pl.ds(0, X - 1)], ag_recv.at[c, 1])
        src = h_buf.at[c, mc]
        for o in range(1, C):
            remote(src, src, ag_send.at[c, 2], ag_recv.at[c, 2],
                   (mz * X + mx) * C + (mc + o) % C).start()

    def head_part(c):
        drain(h_buf.at[c, pl.ds(0, C - 1)], ag_recv.at[c, 2])
        wide = h_buf[c].astype(F32).reshape(n * rows, Nc)
        sq = jnp.sum(wide * wide, axis=1, keepdims=True)
        scaled = (wide * gain[:, c * Nc:(c + 1) * Nc]).astype(BF16)
        hd_copy(c).wait()
        part = jnp.dot(scaled, hd_buf[c], preferred_element_type=F32)
        if c == 0:
            scores[...] = part
            ssq[...] = sq
        else:
            scores[...] += part
            ssq[...] += sq

    stages = [(down, 0.0), (stage2, 2.1), (stage3, 6.1), (gather2, 9.1), (gather3, 11.1), (head_part, 13.1)]
    plan = []
    for c in range(NCH):
        for at, (fn, when) in enumerate(stages):
            plan.append((2.0 * c + when, at, c, fn))
    for _, _, c, fn in sorted(plan, key=lambda item: item[:3]):
        fn(c)

    drain(meta_buf.at[pl.ds(0, n - 1)], mt_recv)
    R = n * rows
    V = scores.shape[1]
    sc = scores[...] * lax.rsqrt(ssq[...] * (1.0 / D) + 1.0)
    ids = meta_buf[...].reshape(R, 128)
    top = jnp.max(sc, axis=1, keepdims=True)
    ex = jnp.exp(sc - top)
    mass = jnp.sum(ex, axis=1, keepdims=True)
    moment = jnp.sum(ex * sc, axis=1, keepdims=True)
    column = iota((R, V), 1) + me * V
    hit = jnp.sum(jnp.where(ids[:, 2:3] == column, sc, 0.0), axis=1, keepdims=True)
    lane = iota((R, 128), 1)
    stat = jnp.where(lane == 0, top, jnp.where(lane == 1, mass, jnp.where(
        lane == 2, moment, jnp.where(lane == 3, hit, 0.0))))
    turned = stat.T[0:8, :]
    st_send[...] = turned
    st_buf[me] = turned

    def stat_send(o, carry):
        remote(st_send, st_buf.at[me], st_ssem, st_rsem, (me + o) % n).start()
        return carry

    lax.fori_loop(1, n, stat_send, 0)

    dom, bins = ids[:, 3:4], ids[:, 4:5]
    col = iota((R, 128), 1)
    spot = (dom - me * DOM_DEV) * BINS + bins
    inside = (dom >= me * DOM_DEV) & (dom < (me + 1) * DOM_DEV)
    own_row = my_place * rows
    hot = ((inside & (col == spot)) | (
        (col >= 64) & (col < 64 + rows) & (iota((R, 128), 0) == own_row + col - 64))).astype(F32)

    for cp in d1:
        cp.wait_send()
    for k in range(1, G):
        drain(recv_d.at[me_g], d2_send.at[k])
    for c in range(NCH):
        for k in range(1, G):
            drain(r1_buf.at[c, k], r1_send.at[c, k])
        drain(r2_buf.at[c, pl.ds(0, E - 1)], r2_send.at[c])
        drain(h_buf.at[c, mc, mx, pl.ds(0, Z - 1)], ag_send.at[c, 0])
        drain(h_buf.at[c, mc, pl.ds(0, X - 1)], ag_send.at[c, 1])
        drain(h_buf.at[c, pl.ds(0, C - 1)], ag_send.at[c, 2])
    drain(meta_buf.at[pl.ds(0, n - 1)], mt_send)
    drain(st_buf.at[pl.ds(0, n - 1)], st_ssem)
    drain(st_buf.at[pl.ds(0, n - 1)], st_rsem)
    tops = st_buf[:, 0, :]
    joined = jnp.max(tops, axis=0, keepdims=True)
    factor = jnp.exp(tops - joined)
    mass_all = jnp.sum(st_buf[:, 1, :] * factor, axis=0, keepdims=True)
    moment_all = jnp.sum(st_buf[:, 2, :] * factor, axis=0, keepdims=True)
    target = jnp.sum(st_buf[:, 3, :], axis=0, keepdims=True)
    log_norm = joined + jnp.log(mass_all)
    nll = log_norm - target
    ent = log_norm - moment_all / mass_all
    kind = iota((8, R), 0)
    vals = jnp.where(kind == 0, 1.0, jnp.where(kind == 1, nll, jnp.where(kind == 2, ent, 0.0)))
    res = jnp.dot(vals, hot, precision=HIGHEST, preferred_element_type=F32)
    out_nll[...] = res[1:2, 64:64 + rows]
    for d in range(DOM_DEV):
        out_table[:, d, :] = res[0:3, d * BINS:(d + 1) * BINS]


def on_device(tokens, router, w_gate, w_up, w_down, norm_gain, head_weight, expert_ids, targets,
              domains, bins):
    n = lax.axis_size("expert")
    rows, D = tokens.shape
    F = w_down.shape[0]
    V = head_weight.shape[1]
    G = n // EXPERTS
    C, X = 2, 2
    Z = n // (C * X)
    TF = 512 if F % 512 == 0 else F
    NF = F // TF
    TD = 512
    ND = D // TD
    NCH = 4
    cfg = dict(n=n, G=G, C=C, X=X, Z=Z, TF=TF, NF=NF, NGU=min(3, NF), TD=TD, ND=ND,
               NDW=min(6, ND), NCH=NCH)
    Nc = D // NCH
    hc = Nc // 2
    vmem = pl.BlockSpec(memory_space=pltpu.VMEM)
    hbm = pl.BlockSpec(memory_space=pltpu.HBM)
    DMA = pltpu.SemaphoreType.DMA
    M = n * PAD
    scratch = [
        pltpu.VMEM((cfg["NGU"], 2, D, TF), BF16),
        pltpu.VMEM((cfg["NDW"], F, TD), BF16),
        pltpu.VMEM((NCH, Nc, V), BF16),
        pltpu.VMEM((EXPERTS, 2 * PAD, D // 2), BF16),
        pltpu.VMEM((G, EXPERTS, 2 * PAD, D // 2), BF16),
        pltpu.VMEM((M, D), BF16),
        pltpu.VMEM((NF, M, TF), BF16),
        pltpu.VMEM((NCH, G, EXPERTS * PAD, Nc), BF16),
        pltpu.VMEM((NCH, G, EXPERTS * PAD, Nc), BF16),
        pltpu.VMEM((NCH, EXPERTS, 2 * PAD, hc), BF16),
        pltpu.VMEM((NCH, EXPERTS, 2 * PAD, hc), BF16),
        pltpu.VMEM((NCH, C, X, Z, rows, Nc), BF16),
        pltpu.VMEM((n, rows, 128), jnp.int32),
        pltpu.VMEM((8, n * rows), F32),
        pltpu.VMEM((n, 8, n * rows), F32),
        pltpu.VMEM((n * rows, V), F32),
        pltpu.VMEM((n * rows, 1), F32),
        pltpu.VMEM((2, rows, EXPERTS * 2 * PAD), F32),
        DMA((cfg["NGU"], 2)), DMA((cfg["NDW"],)), DMA((NCH,)), DMA(()),
        DMA((EXPERTS,)), DMA((EXPERTS,)), DMA((G,)), DMA((G,)),
        DMA((NCH, G)), DMA((NCH, G)), DMA((NCH,)), DMA((NCH,)),
        DMA((NCH, 3)), DMA((NCH, 3)), DMA(()), DMA(()), DMA(()), DMA(()),
    ]
    hidden, nll, table = pl.pallas_call(
        functools.partial(kernel, cfg),
        out_shape=(jax.ShapeDtypeStruct((rows, D), BF16), jax.ShapeDtypeStruct((1, rows), F32),
                   jax.ShapeDtypeStruct((3, DOM_DEV, BINS), F32)),
        in_specs=[vmem] * 7 + [hbm] * 4,
        out_specs=(vmem, vmem, vmem),
        scratch_shapes=scratch,
        compiler_params=pltpu.CompilerParams(
            collective_id=0, has_side_effects=True, vmem_limit_bytes=67043328),
    )(tokens, expert_ids.T, targets[None, :], domains[None, :], bins[None, :], router.T,
      norm_gain[None, :], w_gate, w_up, w_down, head_weight)
    return hidden, nll[0], table


def solution(mesh):
    return jax.shard_map(
        on_device,
        mesh=mesh,
        in_specs=(
            P(("groups", "expert"), None),
            P(),
            P(None, "expert"),
            P(None, "expert"),
            P("expert", None),
            P(),
            P(None, "expert"),
            P(("groups", "expert"), None),
            P(("groups", "expert")),
            P(("groups", "expert")),
            P(("groups", "expert")),
        ),
        out_specs=(
            P(("groups", "expert"), None),
            P(("groups", "expert")),
            P(None, ("groups", "expert"), None),
        ),
        check_vma=False,
    )
```

```python
import functools
import jax
import jax.numpy as jnp
from jax import lax
from jax.experimental import pallas as pl
from jax.experimental.pallas import tpu as pltpu
from jax.sharding import PartitionSpec as P

EXPERTS = 8
DOM_DEV = 2
BINS = 16
CAP = 3
PAD = 4
F32 = jnp.float32
BF16 = jnp.bfloat16
HIGHEST = lax.Precision.HIGHEST


def iota(shape, dim):
    return lax.broadcasted_iota(jnp.int32, shape, dim)


def kernel(cfg, tokens, ids_row, tgt_row, dom_row, bin_row, router_t, gain, w_gate, w_up, w_down,
           head, out_hidden, out_nll, out_table,
           gu_buf, dn_buf, hd_buf, send_d, recv_d, x_buf, act_buf, p_buf, r1_buf, s_buf, r2_buf,
           h_buf, meta_buf, st_send, st_buf, scores, ssq, wt_buf,
           gu_sem, dn_sem, hd_sem, own_sem, d1_send, d1_recv, d2_send, d2_recv, r1_send, r1_recv,
           r2_send, r2_recv, ag_send, ag_recv, mt_send, mt_recv, st_ssem, st_rsem):
    n, G, C, X, Z = cfg["n"], cfg["G"], cfg["C"], cfg["X"], cfg["Z"]
    rows, D = tokens.shape
    half = D // 2
    E = EXPERTS
    TF, NF, NGU = cfg["TF"], cfg["NF"], cfg["NGU"]
    TD, ND, NDW = cfg["TD"], cfg["ND"], cfg["NDW"]
    NCH = cfg["NCH"]
    Nc = D // NCH
    hc = Nc // 2
    per_chunk = ND // NCH
    me = lax.axis_index("expert")
    me_e, me_g = me // G, me % G
    mz, mx, mc = me // (C * X), (me // C) % X, me % C
    my_place = (mc * X + mx) * Z + mz

    def remote(src, dst, ss, rs, peer):
        return pltpu.make_async_remote_copy(
            src_ref=src, dst_ref=dst, send_sem=ss, recv_sem=rs,
            device_id={"expert": peer}, device_id_type=pl.DeviceIdType.MESH)

    def drain(ref, sem):
        pltpu.make_async_copy(ref, ref, sem).wait()

    def gu_copy(t, src, which, slot):
        return pltpu.make_async_copy(
            src.at[:, pl.ds(pl.multiple_of(t * TF, TF if TF % 128 == 0 else 1), TF)] if NF > 1 else src,
            gu_buf.at[slot, which], gu_sem.at[slot, which])

    def gu_start(t, slot):
        gu_copy(t, w_gate, 0, slot).start()
        gu_copy(t, w_up, 1, slot).start()

    def dn_copy(t, slot):
        return pltpu.make_async_copy(
            w_down.at[:, pl.ds(t * TD, TD)], dn_buf.at[slot], dn_sem.at[slot])

    def hd_copy(c):
        return pltpu.make_async_copy(head.at[pl.ds(c * Nc, Nc)], hd_buf.at[c], hd_sem.at[c])

    for t in range(NGU):
        gu_start(t, t)
    barrier = pltpu.get_barrier_semaphore()

    def greet(o, carry):
        pl.semaphore_signal(barrier, inc=1, device_id={"expert": (me + o) % n},
                            device_id_type=pl.DeviceIdType.MESH)
        return carry

    lax.fori_loop(1, n, greet, 0)
    for t in range(NDW):
        dn_copy(t, t).start()

    RB = E * 2 * PAD
    r = iota((RB, rows), 0)
    r_e, r_h, r_s = r // (2 * PAD), (r % (2 * PAD)) // PAD, r % PAD
    member = ((ids_row[0:1, :] == r_e) | (ids_row[1:2, :] == r_e)).astype(F32)
    upper = (iota((rows, rows), 0) < iota((rows, rows), 1)).astype(F32)
    slot = jnp.dot(member, upper, preferred_element_type=F32)
    lay = member * (slot == r_s.astype(F32)).astype(F32)
    lay_lo = (lay * (r_h == 0).astype(F32)).astype(BF16)
    lay_hi = (lay * (r_h == 1).astype(F32)).astype(BF16)
    packed = (jnp.dot(lay_lo, tokens[:, :half], preferred_element_type=F32)
              + jnp.dot(lay_hi, tokens[:, half:], preferred_element_type=F32))
    send_d[...] = packed.reshape(E, 2 * PAD, half).astype(BF16)
    eye = iota((rows, rows), 0) == iota((rows, rows), 1)

    def column_of(row):
        wide = jnp.where(eye, row.astype(F32), 0.0)
        return jnp.sum(wide, axis=1, keepdims=True).astype(jnp.int32)

    ids0, ids1 = column_of(ids_row[0:1, :]), column_of(ids_row[1:2, :])
    ml = iota((rows, 128), 1)
    meta_buf[my_place] = jnp.where(ml == 2, column_of(tgt_row[...]), jnp.where(
        ml == 3, column_of(dom_row[...]), jnp.where(ml == 4, column_of(bin_row[...]), 0)))

    pl.semaphore_wait(barrier, n - 1)

    d1 = []
    for o in range(1, E):
        e = (me_e + o) % E
        cp = remote(send_d.at[e], recv_d.at[me_g, me_e], d1_send.at[o], d1_recv.at[o], e * G + me_g)
        cp.start()
        d1.append(cp)
    own = pltpu.make_async_copy(send_d.at[me_e], recv_d.at[me_g, me_e], own_sem)
    own.start()

    def meta_send(o, carry):
        remote(meta_buf.at[my_place], meta_buf.at[my_place], mt_send, mt_recv, (me + o) % n).start()
        return carry

    tok32 = tokens[...].astype(F32)
    c0 = jnp.zeros((rows, 1), F32)
    c1 = jnp.zeros((rows, 1), F32)
    for e in range(E):
        logit = jnp.sum(tok32 * router_t[e:e + 1, :], axis=1, keepdims=True)
        c0 = c0 + jnp.where(ids0 == e, logit, 0.0)
        c1 = c1 + jnp.where(ids1 == e, logit, 0.0)
    g0 = 1.0 / (1.0 + jnp.exp(c1 - c0))
    g1 = 1.0 / (1.0 + jnp.exp(c0 - c1))
    q = iota((rows, RB), 1)
    q_e, q_h, q_s = q // (2 * PAD), (q % (2 * PAD)) // PAD, q % PAD
    is0, is1 = ids0 == q_e, ids1 == q_e
    member_t = (is0 | is1).astype(F32)
    lower = (iota((rows, rows), 1) < iota((rows, rows), 0)).astype(F32)
    slot_t = jnp.dot(lower, member_t, preferred_element_type=F32)
    weight = (jnp.where(is0, g0, 0.0) + jnp.where(is1, g1, 0.0)) * (
        slot_t == q_s.astype(F32)).astype(F32)
    wt_buf[0] = weight * (q_h == 0).astype(F32)
    wt_buf[1] = weight * (q_h == 1).astype(F32)

    own.wait()
    d2 = []
    for o in range(E):
        e = (me_e - o + E) % E
        if o > 0:
            d1[o - 1].wait_recv()
        for k in range(1, G):
            cp = remote(recv_d.at[me_g, e], recv_d.at[me_g, e], d2_send.at[k], d2_recv.at[k],
                        me_e * G + (me_g + k) % G)
            cp.start()
    for k in range(1, G):
        drain(recv_d.at[(me_g - k + G) % G], d2_recv.at[k])

    M = n * PAD
    pick_r, pick_c = iota((M, n * 2 * PAD), 0), iota((M, n * 2 * PAD), 1)
    base = (pick_r // PAD) * (2 * PAD) + pick_r % PAD
    sel_lo = (pick_c == base).astype(BF16)
    sel_hi = (pick_c == base + PAD).astype(BF16)
    W = 512
    for j in range(half // W):
        got = recv_d[:, :, :, j * W:(j + 1) * W].astype(F32).reshape(n * 2 * PAD, W).astype(BF16)
        x_buf[:, j * W:(j + 1) * W] = jnp.dot(
            sel_lo, got, preferred_element_type=F32).astype(BF16)
        x_buf[:, half + j * W:half + (j + 1) * W] = jnp.dot(
            sel_hi, got, preferred_element_type=F32).astype(BF16)

    lax.fori_loop(1, n, meta_send, 0)

    def expert_tile(t, carry):
        s = t % NGU
        gu_copy(t, w_gate, 0, s).wait()
        g = jnp.dot(x_buf[...], gu_buf[s, 0], preferred_element_type=F32)
        gu_copy(t, w_up, 1, s).wait()
        u = jnp.dot(x_buf[...], gu_buf[s, 1], preferred_element_type=F32)
        a = (g / (1.0 + jnp.exp(-g)) * u).astype(BF16)
        act_buf[t] = a

        @pl.when(t + NGU < NF)
        def _():
            gu_start(t + NGU, s)

        return carry

    lax.fori_loop(0, NF, expert_tile, 0)

    br = iota((RB, E * PAD), 0)
    bc = iota((RB, E * PAD), 1)
    b_src = (br // (2 * PAD)) * PAD + br % PAD
    b_h = (br % (2 * PAD)) // PAD
    blk_lo = ((bc == b_src) & (b_h == 0)).astype(BF16)
    blk_hi = ((bc == b_src) & (b_h == 1)).astype(BF16)

    def down(c):
        for i in range(per_chunk):
            t = c * per_chunk + i
            s = t % NDW
            dn_copy(t, s).wait()
            acc = jnp.dot(act_buf[0], dn_buf[s, 0:TF], preferred_element_type=F32)
            for f in range(1, NF):
                acc = acc + jnp.dot(act_buf[f], dn_buf[s, f * TF:(f + 1) * TF],
                                    preferred_element_type=F32)
            p_buf[c, :, :, i * TD:(i + 1) * TD] = acc.astype(BF16).reshape(G, E * PAD, TD)
            if t + NDW < ND:
                dn_copy(t + NDW, s).start()
            if t + 1 == max(ND - NDW, 1):
                for h in range(NCH):
                    hd_copy(h).start()
        for k in range(1, G):
            remote(p_buf.at[c, (me_g + k) % G], r1_buf.at[c, k], r1_send.at[c, k], r1_recv.at[c, k],
                   me_e * G + (me_g + k) % G).start()

    def stage2(c):
        total = p_buf[c, me_g].astype(F32)
        for k in range(1, G):
            drain(r1_buf.at[c, k], r1_recv.at[c, k])
            total = total + r1_buf[c, k].astype(F32)
        summed = total.astype(BF16)
        block = (jnp.dot(blk_lo, summed[:, :hc], preferred_element_type=F32)
                 + jnp.dot(blk_hi, summed[:, hc:], preferred_element_type=F32))
        s_buf[c] = block.reshape(E, 2 * PAD, hc).astype(BF16)
        r2_buf[c, me_e] = s_buf[c, me_e]
        for o in range(1, E):
            e = (me_e + o) % E
            remote(s_buf.at[c, e], r2_buf.at[c, me_e], r2_send.at[c], r2_recv.at[c],
                   e * G + me_g).start()

    def stage3(c):
        drain(r2_buf.at[c, pl.ds(0, E - 1)], r2_recv.at[c])
        got = r2_buf[c].astype(F32).reshape(RB, hc)
        at = c * Nc
        for h in range(2):
            moe = jnp.dot(wt_buf[h], got, precision=HIGHEST, preferred_element_type=F32)
            lo = at + h * hc
            hid = (tokens[:, lo:lo + hc].astype(F32) + moe).astype(BF16)
            out_hidden[:, lo:lo + hc] = hid
            h_buf[c, mc, mx, mz, :, h * hc:(h + 1) * hc] = hid
        src = h_buf.at[c, mc, mx, mz]
        for o in range(1, Z):
            remote(src, src, ag_send.at[c, 0], ag_recv.at[c, 0],
                   (((mz + o) % Z) * X + mx) * C + mc).start()

    def gather2(c):
        drain(h_buf.at[c, mc, mx, pl.ds(0, Z - 1)], ag_recv.at[c, 0])
        src = h_buf.at[c, mc, mx]
        for o in range(1, X):
            remote(src, src, ag_send.at[c, 1], ag_recv.at[c, 1],
                   (mz * X + (mx + o) % X) * C + mc).start()

    def gather3(c):
        drain(h_buf.at[c, mc, pl.ds(0, X - 1)], ag_recv.at[c, 1])
        src = h_buf.at[c, mc]
        for o in range(1, C):
            remote(src, src, ag_send.at[c, 2], ag_recv.at[c, 2],
                   (mz * X + mx) * C + (mc + o) % C).start()

    def head_part(c):
        drain(h_buf.at[c, pl.ds(0, C - 1)], ag_recv.at[c, 2])
        wide = h_buf[c].astype(F32).reshape(n * rows, Nc)
        sq = jnp.sum(wide * wide, axis=1, keepdims=True)
        scaled = (wide * gain[:, c * Nc:(c + 1) * Nc]).astype(BF16)
        hd_copy(c).wait()
        part = jnp.dot(scaled, hd_buf[c], preferred_element_type=F32)
        if c == 0:
            scores[...] = part
            ssq[...] = sq
        else:
            scores[...] += part
            ssq[...] += sq

    stages = [(down, 0.0), (stage2, 2.1), (stage3, 8.2), (gather2, 11.1), (gather3, 13.1), (head_part, 15.1)]
    plan = []
    for c in range(NCH):
        for at, (fn, when) in enumerate(stages):
            plan.append((2.0 * c + when, at, c, fn))
    for _, _, c, fn in sorted(plan, key=lambda item: item[:3]):
        fn(c)

    drain(meta_buf.at[pl.ds(0, n - 1)], mt_recv)
    R = n * rows
    V = scores.shape[1]
    sc = scores[...] * lax.rsqrt(ssq[...] * (1.0 / D) + 1.0)
    ids = meta_buf[...].reshape(R, 128)
    top = jnp.max(sc, axis=1, keepdims=True)
    ex = jnp.exp(sc - top)
    mass = jnp.sum(ex, axis=1, keepdims=True)
    moment = jnp.sum(ex * sc, axis=1, keepdims=True)
    column = iota((R, V), 1) + me * V
    hit = jnp.sum(jnp.where(ids[:, 2:3] == column, sc, 0.0), axis=1, keepdims=True)
    lane = iota((R, 128), 1)
    stat = jnp.where(lane == 0, top, jnp.where(lane == 1, mass, jnp.where(
        lane == 2, moment, jnp.where(lane == 3, hit, 0.0))))
    turned = stat.T[0:8, :]
    st_send[...] = turned
    st_buf[me] = turned

    def stat_send(o, carry):
        remote(st_send, st_buf.at[me], st_ssem, st_rsem, (me + o) % n).start()
        return carry

    lax.fori_loop(1, n, stat_send, 0)

    dom, bins = ids[:, 3:4], ids[:, 4:5]
    col = iota((R, 128), 1)
    spot = (dom - me * DOM_DEV) * BINS + bins
    inside = (dom >= me * DOM_DEV) & (dom < (me + 1) * DOM_DEV)
    own_row = my_place * rows
    hot = ((inside & (col == spot)) | (
        (col >= 64) & (col < 64 + rows) & (iota((R, 128), 0) == own_row + col - 64))).astype(F32)

    for cp in d1:
        cp.wait_send()
    for k in range(1, G):
        drain(recv_d.at[me_g], d2_send.at[k])
    for c in range(NCH):
        for k in range(1, G):
            drain(r1_buf.at[c, k], r1_send.at[c, k])
        drain(r2_buf.at[c, pl.ds(0, E - 1)], r2_send.at[c])
        drain(h_buf.at[c, mc, mx, pl.ds(0, Z - 1)], ag_send.at[c, 0])
        drain(h_buf.at[c, mc, pl.ds(0, X - 1)], ag_send.at[c, 1])
        drain(h_buf.at[c, pl.ds(0, C - 1)], ag_send.at[c, 2])
    drain(meta_buf.at[pl.ds(0, n - 1)], mt_send)
    drain(st_buf.at[pl.ds(0, n - 1)], st_ssem)
    drain(st_buf.at[pl.ds(0, n - 1)], st_rsem)
    tops = st_buf[:, 0, :]
    joined = jnp.max(tops, axis=0, keepdims=True)
    factor = jnp.exp(tops - joined)
    mass_all = jnp.sum(st_buf[:, 1, :] * factor, axis=0, keepdims=True)
    moment_all = jnp.sum(st_buf[:, 2, :] * factor, axis=0, keepdims=True)
    target = jnp.sum(st_buf[:, 3, :], axis=0, keepdims=True)
    log_norm = joined + jnp.log(mass_all)
    nll = log_norm - target
    ent = log_norm - moment_all / mass_all
    kind = iota((8, R), 0)
    vals = jnp.where(kind == 0, 1.0, jnp.where(kind == 1, nll, jnp.where(kind == 2, ent, 0.0)))
    res = jnp.dot(vals, hot, precision=HIGHEST, preferred_element_type=F32)
    out_nll[...] = res[1:2, 64:64 + rows]
    for d in range(DOM_DEV):
        out_table[:, d, :] = res[0:3, d * BINS:(d + 1) * BINS]


def on_device(tokens, router, w_gate, w_up, w_down, norm_gain, head_weight, expert_ids, targets,
              domains, bins):
    n = lax.axis_size("expert")
    rows, D = tokens.shape
    F = w_down.shape[0]
    V = head_weight.shape[1]
    G = n // EXPERTS
    C, X = 2, 2
    Z = n // (C * X)
    TF = 512 if F % 512 == 0 else F
    NF = F // TF
    TD = 512
    ND = D // TD
    NCH = 4
    cfg = dict(n=n, G=G, C=C, X=X, Z=Z, TF=TF, NF=NF, NGU=min(3, NF), TD=TD, ND=ND,
               NDW=min(6, ND), NCH=NCH)
    Nc = D // NCH
    hc = Nc // 2
    vmem = pl.BlockSpec(memory_space=pltpu.VMEM)
    hbm = pl.BlockSpec(memory_space=pltpu.HBM)
    DMA = pltpu.SemaphoreType.DMA
    M = n * PAD
    scratch = [
        pltpu.VMEM((cfg["NGU"], 2, D, TF), BF16),
        pltpu.VMEM((cfg["NDW"], F, TD), BF16),
        pltpu.VMEM((NCH, Nc, V), BF16),
        pltpu.VMEM((EXPERTS, 2 * PAD, D // 2), BF16),
        pltpu.VMEM((G, EXPERTS, 2 * PAD, D // 2), BF16),
        pltpu.VMEM((M, D), BF16),
        pltpu.VMEM((NF, M, TF), BF16),
        pltpu.VMEM((NCH, G, EXPERTS * PAD, Nc), BF16),
        pltpu.VMEM((NCH, G, EXPERTS * PAD, Nc), BF16),
        pltpu.VMEM((NCH, EXPERTS, 2 * PAD, hc), BF16),
        pltpu.VMEM((NCH, EXPERTS, 2 * PAD, hc), BF16),
        pltpu.VMEM((NCH, C, X, Z, rows, Nc), BF16),
        pltpu.VMEM((n, rows, 128), jnp.int32),
        pltpu.VMEM((8, n * rows), F32),
        pltpu.VMEM((n, 8, n * rows), F32),
        pltpu.VMEM((n * rows, V), F32),
        pltpu.VMEM((n * rows, 1), F32),
        pltpu.VMEM((2, rows, EXPERTS * 2 * PAD), F32),
        DMA((cfg["NGU"], 2)), DMA((cfg["NDW"],)), DMA((NCH,)), DMA(()),
        DMA((EXPERTS,)), DMA((EXPERTS,)), DMA((G,)), DMA((G,)),
        DMA((NCH, G)), DMA((NCH, G)), DMA((NCH,)), DMA((NCH,)),
        DMA((NCH, 3)), DMA((NCH, 3)), DMA(()), DMA(()), DMA(()), DMA(()),
    ]
    hidden, nll, table = pl.pallas_call(
        functools.partial(kernel, cfg),
        out_shape=(jax.ShapeDtypeStruct((rows, D), BF16), jax.ShapeDtypeStruct((1, rows), F32),
                   jax.ShapeDtypeStruct((3, DOM_DEV, BINS), F32)),
        in_specs=[vmem] * 7 + [hbm] * 4,
        out_specs=(vmem, vmem, vmem),
        scratch_shapes=scratch,
        compiler_params=pltpu.CompilerParams(
            collective_id=0, has_side_effects=True, vmem_limit_bytes=67043328),
    )(tokens, expert_ids.T, targets[None, :], domains[None, :], bins[None, :], router.T,
      norm_gain[None, :], w_gate, w_up, w_down, head_weight)
    return hidden, nll[0], table


def solution(mesh):
    return jax.shard_map(
        on_device,
        mesh=mesh,
        in_specs=(
            P(("groups", "expert"), None),
            P(),
            P(None, "expert"),
            P(None, "expert"),
            P("expert", None),
            P(),
            P(None, "expert"),
            P(("groups", "expert"), None),
            P(("groups", "expert")),
            P(("groups", "expert")),
            P(("groups", "expert")),
        ),
        out_specs=(
            P(("groups", "expert"), None),
            P(("groups", "expert")),
            P(None, ("groups", "expert"), None),
        ),
        check_vma=False,
    )
```
